16 devices in a mesh: dp: 2 (over y, z), tp: 8 (over x, core).
Axes of the slice: x: 4, y: 2, z: 1, core: 2. Of those that a mesh axis runs over, the one named last changes fastest.
The devices are a block of a 4x4x8 slice.
Arguments:
- tokens: int32 [6, 1536], P('dp'), parts along dimension 0
- positions: int32 [6, 1536], P('dp'), parts along dimension 0
- embed_table: bfloat16 [32000, 4096], P('tp')
- w_query: bfloat16 [4096, 32, 128], P(None, 'tp')
- w_key: bfloat16 [4096, 8, 128], P(None, 'tp')
- w_value: bfloat16 [4096, 8, 128], P(None, 'tp')
- w_out: bfloat16 [32, 128, 4096], P('tp')
- w_gate: bfloat16 [4096, 14336], P(None, 'tp')
- w_up: bfloat16 [4096, 14336], P(None, 'tp')
- w_down: bfloat16 [14336, 4096], P('tp')
- norm_pre_att: float32 [4096], replicated
- norm_post_att: float32 [4096], replicated
- norm_pre_ffw: float32 [4096], replicated
- norm_post_ffw: float32 [4096], replicated
Outputs:
- output: bfloat16 [6, 1536, 4096], P('dp', 'tp'), parts along dimension 0
There are 2 independent parts. The reference program is written for one: setup_inputs(seed, part) draws one part's arguments, and reference() takes and returns one part's arrays. A program takes and returns all parts, laid end to end along the dimension named above; an argument that names none is the same for every part.
All inputs are finite; a program needn't handle non-finite values.
Results may differ from the reference program's by a relative error of at most 0.0181964.
Values are sent between devices in bfloat16 or wider.
A program may use at most 768 MiB of HBM per device.

```python
import jax
import jax.numpy as jnp
from jax import lax

BATCH_SIZE = 3
SEQ_LEN = 1536
MODEL_DIM = 4096
N_HEADS = 32
KV_HEADS = 8
HEAD_DIM = 128
FFN_DIM = 14336
VOCAB_SIZE = 32000
WINDOW = 4096
QUERY_SCALAR = 256

GROUP_SIZE = N_HEADS // KV_HEADS
QUERY_BLOCK = min(128, SEQ_LEN)
KEY_SPAN = min(SEQ_LEN, WINDOW + QUERY_BLOCK)
SOFT_CAP = 50.0
NORM_EPS = 1e-6
ROPE_BASE = 10000.0


def setup_inputs(seed: int = 0, part: int = 0) -> dict:
    root_key = jax.random.key(seed)
    key_list = jax.random.split(root_key, 11)
    part_keys = jax.random.split(jax.random.fold_in(root_key, part), 5)
    grid_shape = (BATCH_SIZE, SEQ_LEN)
    choice = jax.random.randint(part_keys[0], grid_shape, 0, 4, dtype=jnp.int32)
    hot_ids = jax.random.randint(part_keys[1], grid_shape, 0, VOCAB_SIZE // 4, dtype=jnp.int32)
    any_ids = jax.random.randint(part_keys[2], grid_shape, 0, VOCAB_SIZE, dtype=jnp.int32)
    tokens = jnp.where(choice < 3, hot_ids, any_ids)
    tokens = tokens.at[0, 0].set(VOCAB_SIZE - 1).at[0, 1].set(0)
    pos_step = max(1, (2 * WINDOW) // SEQ_LEN)
    pos_gaps = jax.random.randint(part_keys[3], grid_shape, 1, 2 * pos_step + 1, dtype=jnp.int32)
    first_pos = jax.random.randint(part_keys[4], (BATCH_SIZE, 1), 0, WINDOW, dtype=jnp.int32)
    positions = (first_pos + jnp.cumsum(pos_gaps, axis=1) - pos_gaps[:, :1]).astype(jnp.int32)

    def draw_weight(key_index, w_shape, fan_in):
        raw_noise = jax.random.normal(key_list[key_index], w_shape, jnp.float32)
        return (raw_noise * fan_in ** -0.5).astype(jnp.bfloat16)

    def table_rows(row_group):
        raw_noise = jax.random.normal(jax.random.fold_in(key_list[0], row_group), (VOCAB_SIZE // 8, MODEL_DIM), jnp.float32)
        return (raw_noise * MODEL_DIM ** -0.5).astype(jnp.bfloat16)

    embed_table = lax.map(table_rows, jnp.arange(8)).reshape(VOCAB_SIZE, MODEL_DIM)
    norm_draws = 0.3 * jax.random.normal(key_list[8], (4, MODEL_DIM), jnp.float32)
    return {
        "tokens": tokens,
        "positions": positions,
        "embed_table": embed_table,
        "w_query": draw_weight(1, (MODEL_DIM, N_HEADS, HEAD_DIM), MODEL_DIM),
        "w_key": draw_weight(2, (MODEL_DIM, KV_HEADS, HEAD_DIM), MODEL_DIM),
        "w_value": draw_weight(3, (MODEL_DIM, KV_HEADS, HEAD_DIM), MODEL_DIM),
        "w_out": draw_weight(4, (N_HEADS, HEAD_DIM, MODEL_DIM), N_HEADS * HEAD_DIM),
        "w_gate": draw_weight(5, (MODEL_DIM, FFN_DIM), MODEL_DIM),
        "w_up": draw_weight(6, (MODEL_DIM, FFN_DIM), MODEL_DIM),
        "w_down": draw_weight(7, (FFN_DIM, MODEL_DIM), FFN_DIM),
        "norm_pre_att": norm_draws[0],
        "norm_post_att": norm_draws[1],
        "norm_pre_ffw": norm_draws[2],
        "norm_post_ffw": norm_draws[3],
    }


def rms_norm(hidden, norm_scale):
    hidden = hidden.astype(jnp.float32)
    mean_sq = jnp.mean(hidden * hidden, axis=-1, keepdims=True)
    return (hidden * lax.rsqrt(mean_sq + NORM_EPS) * (1.0 + norm_scale)).astype(jnp.bfloat16)


def apply_rope(states, positions):
    half_dim = HEAD_DIM // 2
    inv_freq = ROPE_BASE ** (-2.0 * jnp.arange(half_dim, dtype=jnp.float32) / HEAD_DIM)
    angles = positions.astype(jnp.float32)[:, :, None] * inv_freq
    cos_tab = jnp.cos(angles)[:, :, None, :]
    sin_tab = jnp.sin(angles)[:, :, None, :]
    lower_half = states[..., :half_dim]
    upper_half = states[..., half_dim:]
    return jnp.concatenate([lower_half * cos_tab - upper_half * sin_tab, upper_half * cos_tab + lower_half * sin_tab], axis=-1)


def project(act_rows, weight, out_shape):
    flat_rows = act_rows.reshape(-1, act_rows.shape[-1])
    flat_w = weight.reshape(act_rows.shape[-1], -1)
    return jnp.dot(flat_rows, flat_w, preferred_element_type=jnp.float32).reshape(out_shape)


def attend(q_states, k_states, v_states, positions):
    n_blocks = SEQ_LEN // QUERY_BLOCK

    def one_block(block_idx):
        q_start = block_idx * QUERY_BLOCK
        k_start = jnp.maximum(q_start + QUERY_BLOCK - KEY_SPAN, 0)
        q_blk = lax.dynamic_slice_in_dim(q_states, q_start, QUERY_BLOCK, axis=1)
        k_blk = lax.dynamic_slice_in_dim(k_states, k_start, KEY_SPAN, axis=1)
        v_blk = lax.dynamic_slice_in_dim(v_states, k_start, KEY_SPAN, axis=1)
        q_pos = lax.dynamic_slice_in_dim(positions, q_start, QUERY_BLOCK, axis=1)
        k_pos = lax.dynamic_slice_in_dim(positions, k_start, KEY_SPAN, axis=1)
        scores = jnp.einsum("bqkgd,blkd->bkgql", q_blk.astype(jnp.float32), k_blk.astype(jnp.float32))
        capped = SOFT_CAP * jnp.tanh(scores / SOFT_CAP)
        offset = q_pos[:, :, None] - k_pos[:, None, :]
        keep_mask = (offset >= 0) & (offset < WINDOW)
        capped = jnp.where(keep_mask[:, None, None, :, :], capped, -1e30)
        att_probs = jax.nn.softmax(capped, axis=-1).astype(jnp.bfloat16)
        att_mix = jnp.einsum("bkgql,blkd->bqkgd", att_probs.astype(jnp.float32), v_blk.astype(jnp.float32))
        return att_mix.astype(jnp.bfloat16)

    blocks = lax.map(one_block, jnp.arange(n_blocks))
    return jnp.moveaxis(blocks, 0, 1).reshape(BATCH_SIZE, SEQ_LEN, KV_HEADS, GROUP_SIZE, HEAD_DIM)


def reference(tokens, positions, embed_table, w_query, w_key, w_value, w_out, w_gate, w_up, w_down, norm_pre_att, norm_post_att, norm_pre_ffw, norm_post_ffw):
    normalizer = jnp.sqrt(jnp.float32(MODEL_DIM)).astype(jnp.bfloat16).astype(jnp.float32)
    looked = jnp.take(embed_table, tokens, axis=0)
    embeds = (looked.astype(jnp.float32) * normalizer).astype(jnp.bfloat16)
    attn_in = rms_norm(embeds, norm_pre_att)
    heads_shape = (BATCH_SIZE, SEQ_LEN, N_HEADS, HEAD_DIM)
    kv_shape = (BATCH_SIZE, SEQ_LEN, KV_HEADS, HEAD_DIM)
    q_states = apply_rope(project(attn_in, w_query, heads_shape), positions) * QUERY_SCALAR ** -0.5
    q_states = q_states.astype(jnp.bfloat16).reshape(BATCH_SIZE, SEQ_LEN, KV_HEADS, GROUP_SIZE, HEAD_DIM)
    k_states = apply_rope(project(attn_in, w_key, kv_shape), positions).astype(jnp.bfloat16)
    v_states = project(attn_in, w_value, kv_shape).astype(jnp.bfloat16)
    att_mix = attend(q_states, k_states, v_states, positions)
    model_shape = (BATCH_SIZE, SEQ_LEN, MODEL_DIM)
    att_flat = att_mix.reshape(BATCH_SIZE, SEQ_LEN, N_HEADS * HEAD_DIM)
    att_proj = project(att_flat, w_out, model_shape).astype(jnp.bfloat16)
    resid_one = (embeds.astype(jnp.float32) + rms_norm(att_proj, norm_post_att).astype(jnp.float32)).astype(jnp.bfloat16)
    mlp_in = rms_norm(resid_one, norm_pre_ffw)
    ffn_shape = (BATCH_SIZE, SEQ_LEN, FFN_DIM)
    gate_pre = project(mlp_in, w_gate, ffn_shape)
    up_proj = project(mlp_in, w_up, ffn_shape)
    ffn_act = (jax.nn.gelu(gate_pre, approximate=True) * up_proj).astype(jnp.bfloat16)
    down_proj = project(ffn_act, w_down, model_shape).astype(jnp.bfloat16)
    return (resid_one.astype(jnp.float32) + rms_norm(down_proj, norm_post_ffw).astype(jnp.float32)).astype(jnp.bfloat16)
```

```python
import functools

import jax
import jax.numpy as jnp
from jax import lax
from jax.experimental import pallas as pl
from jax.experimental.pallas import tpu as pltpu
from jax.sharding import PartitionSpec as P

WINDOW = 4096
QUERY_SCALE = 256.0 ** -0.5
SOFT_CAP = 50.0
NORM_EPS = 1e-6
ROPE_BASE = 10000.0


def rms_norm(hidden, norm_scale):
    hidden = hidden.astype(jnp.float32)
    mean_sq = jnp.mean(hidden * hidden, axis=-1, keepdims=True)
    return (hidden * lax.rsqrt(mean_sq + NORM_EPS) * (1.0 + norm_scale)).astype(jnp.bfloat16)


def rope_tables(positions, head_dim):
    half_dim = head_dim // 2
    inv_freq = ROPE_BASE ** (-2.0 * jnp.arange(half_dim, dtype=jnp.float32) / head_dim)
    angles = positions.astype(jnp.float32)[:, :, None] * inv_freq
    cos_tab, sin_tab = jnp.cos(angles), jnp.sin(angles)
    return jnp.concatenate([cos_tab, cos_tab], axis=-1), jnp.concatenate([-sin_tab, sin_tab], axis=-1)


def attention_body(q_block, pos_row_ref, pos_col_ref, q_ref, k_ref, v_ref, cos_ref, sin_ref, out_ref):
    seq_len, head_dim = q_ref.shape
    half_dim = head_dim // 2

    def rope(states):
        return states * cos_ref[...] + pltpu.roll(states, half_dim, 1) * sin_ref[...]

    keys = rope(k_ref[...]).astype(jnp.bfloat16)
    values = v_ref[...].astype(jnp.bfloat16)
    queries = (rope(q_ref[...]) * QUERY_SCALE).astype(jnp.bfloat16)
    for start in range(0, seq_len, q_block):
        span = start + q_block
        scores = lax.dot_general(queries[start:span], keys[:span], (((1,), (1,)), ((), ())), preferred_element_type=jnp.float32)
        capped = SOFT_CAP * jnp.tanh(scores * (1.0 / SOFT_CAP))
        offset = pos_col_ref[start:span, :] - pos_row_ref[:, :span]
        keep_mask = (offset >= 0) & (offset < WINDOW)
        weights = jnp.where(keep_mask, jnp.exp(capped), 0.0)
        total = jnp.sum(weights, axis=-1, keepdims=True)
        probs = (weights * (1.0 / total)).astype(jnp.bfloat16)
        mix = jnp.dot(probs, values[:span], preferred_element_type=jnp.float32)
        out_ref[start:span, :] = mix.astype(jnp.bfloat16)


def local_attention(qkv, positions, cos_tab, sin_tab, n_heads, head_dim, kv_local):
    seq_len = qkv.shape[0]
    n_group = n_heads // kv_local
    whole = pl.BlockSpec((seq_len, head_dim), lambda h: (0, 0))
    flops = 2 * n_heads * seq_len * seq_len * head_dim * 2
    return pl.pallas_call(
        functools.partial(attention_body, 256),
        grid=(n_heads,),
        in_specs=[
            pl.BlockSpec((1, seq_len), lambda h: (0, 0)),
            pl.BlockSpec((seq_len, 1), lambda h: (0, 0)),
            pl.BlockSpec((seq_len, head_dim), lambda h: (0, h)),
            pl.BlockSpec((seq_len, head_dim), lambda h: (0, n_heads + h // n_group)),
            pl.BlockSpec((seq_len, head_dim), lambda h: (0, n_heads + kv_local + h // n_group)),
            whole,
            whole,
        ],
        out_specs=pl.BlockSpec((seq_len, head_dim), lambda h: (0, h)),
        out_shape=jax.ShapeDtypeStruct((seq_len, n_heads * head_dim), jnp.bfloat16),
        compiler_params=pltpu.CompilerParams(vmem_limit_bytes=40 * 1024 * 1024),
        cost_estimate=pl.CostEstimate(flops=flops, bytes_accessed=12 * seq_len * n_heads * head_dim, transcendentals=0),
        name="attention",
    )(positions[None, :], positions[:, None], qkv, qkv, qkv, cos_tab, sin_tab)


def solution(mesh):
    in_specs = (P("dp", None), P("dp", None), P("tp", None), P(None, "tp", None), P(None, "tp", None), P(None, "tp", None), P("tp", None, None), P(None, "tp"), P(None, "tp"), P("tp", None), P(None), P(None), P(None), P(None))
    n_dev = mesh.shape["tp"]
    n_chip = n_dev // 2
    to_right = [(i, (i + 2) % n_dev) for i in range(n_dev)]
    to_left = [(i, (i - 2) % n_dev) for i in range(n_dev)]
    to_partner = [(i, i ^ 1) for i in range(n_dev)]

    def device_step(tokens, positions, embed_block, w_query, w_key, w_value, w_out, w_gate, w_up, w_down, norm_pre_att, norm_post_att, norm_pre_ffw, norm_post_ffw):
        dev_rank = lax.axis_index("tp")
        chip, core = dev_rank // 2, dev_rank % 2
        vocab_local, model_dim = embed_block.shape
        n_batch, seq_len = tokens.shape
        chunk = seq_len // n_dev
        half = chunk // 2
        n_heads, head_dim = w_query.shape[1], w_query.shape[2]
        kv_local = w_key.shape[1]

        def by_parity(rows):
            split = rows.reshape((n_chip, 2, chunk) + rows.shape[1:])
            other = lax.dynamic_index_in_dim(split, 1 - core, 1, keepdims=False)
            own = lax.dynamic_index_in_dim(split, core, 1, keepdims=False)
            return own.reshape((n_chip * chunk,) + rows.shape[1:]), other.reshape((n_chip * chunk,) + rows.shape[1:])

        def reduce_scatter(part_fn, rows):
            own_rows, other_rows = by_parity(rows)
            other = part_fn(other_rows)
            from_partner = lax.ppermute(other, "tp", to_partner)
            own = part_fn(own_rows)

            def pair_sum(step, upper):
                start = ((chip + step) % n_chip) * chunk + (half if upper else 0)
                mine = lax.dynamic_slice_in_dim(own, start, half, 0)
                theirs = lax.dynamic_slice_in_dim(from_partner, start, half, 0)
                return mine.astype(jnp.float32) + theirs.astype(jnp.float32)

            far_low = lax.ppermute(pair_sum(2, False).astype(jnp.bfloat16), "tp", to_right)
            far_high = lax.ppermute(pair_sum(2, True).astype(jnp.bfloat16), "tp", to_left)
            left_high = lax.ppermute(pair_sum(1, True).astype(jnp.bfloat16), "tp", to_right)
            right_low = lax.ppermute(pair_sum(n_chip - 1, False).astype(jnp.bfloat16), "tp", to_left)
            left_low = lax.ppermute((pair_sum(1, False) + far_low.astype(jnp.float32)).astype(jnp.bfloat16), "tp", to_right)
            right_high = lax.ppermute((pair_sum(n_chip - 1, True) + far_high.astype(jnp.float32)).astype(jnp.bfloat16), "tp", to_left)
            low = pair_sum(0, False) + right_low.astype(jnp.float32) + left_low.astype(jnp.float32)
            high = pair_sum(0, True) + left_high.astype(jnp.float32) + right_high.astype(jnp.float32)
            return jnp.concatenate([low, high], axis=0).astype(jnp.bfloat16)

        normalizer = jnp.sqrt(jnp.float32(model_dim)).astype(jnp.bfloat16)

        def lookup(ids):
            local_ids = ids - dev_rank * vocab_local
            in_block = (local_ids >= 0) & (local_ids < vocab_local)
            looked = jnp.take(embed_block, jnp.clip(local_ids, 0, vocab_local - 1), axis=0)
            return jnp.where(in_block[:, None], looked * normalizer, jnp.zeros((), jnp.bfloat16))

        w_qkv = jnp.concatenate([w.reshape(model_dim, -1) for w in (w_query, w_key, w_value)], axis=1)
        w_out_flat = w_out.reshape(-1, model_dim)
        cos_tab, sin_tab = rope_tables(positions, head_dim)

        def project_out(rows):
            return jnp.dot(rows, w_out_flat, preferred_element_type=jnp.float32).astype(jnp.bfloat16)

        def project_down(rows):
            return jnp.dot(rows, w_down, preferred_element_type=jnp.float32).astype(jnp.bfloat16)

        outs = []
        for b in range(n_batch):
            embeds = reduce_scatter(lookup, tokens[b])
            attn_in = lax.all_gather(rms_norm(embeds, norm_pre_att), "tp", axis=0, tiled=True)
            qkv = jnp.dot(attn_in, w_qkv, preferred_element_type=jnp.float32)
            att_mix = local_attention(qkv, positions[b], cos_tab[b], sin_tab[b], n_heads, head_dim, kv_local)
            att_proj = reduce_scatter(project_out, att_mix)
            resid_one = (embeds.astype(jnp.float32) + rms_norm(att_proj, norm_post_att).astype(jnp.float32)).astype(jnp.bfloat16)
            mlp_in = lax.all_gather(rms_norm(resid_one, norm_pre_ffw), "tp", axis=0, tiled=True)
            gate_pre = jnp.dot(mlp_in, w_gate, preferred_element_type=jnp.float32)
            up_proj = jnp.dot(mlp_in, w_up, preferred_element_type=jnp.float32)
            ffn_act = (jax.nn.gelu(gate_pre, approximate=True) * up_proj).astype(jnp.bfloat16)
            down_proj = reduce_scatter(project_down, ffn_act)
            outs.append((resid_one.astype(jnp.float32) + rms_norm(down_proj, norm_post_ffw).astype(jnp.float32)).astype(jnp.bfloat16))
        return jnp.stack(outs)

    return jax.shard_map(device_step, mesh=mesh, in_specs=in_specs, out_specs=P("dp", "tp", None), check_vma=False)
```

```python
import functools

import jax
import jax.numpy as jnp
from jax import lax
from jax.experimental import pallas as pl
from jax.experimental.pallas import tpu as pltpu
from jax.sharding import PartitionSpec as P


WINDOW = 4096
QUERY_SCALE = 256.0 ** -0.5
SOFT_CAP = 50.0
NORM_EPS = 1e-6
ROPE_BASE = 10000.0

ROW_ORDER = "000101120212100000021012111010012222202121110210221220122"


def step_order(n_batch):
    return [int(row) for row in ROW_ORDER if int(row) < n_batch]


def rms_norm(hidden, norm_scale):
    hidden = hidden.astype(jnp.float32)
    mean_sq = jnp.mean(hidden * hidden, axis=-1, keepdims=True)
    return (hidden * lax.rsqrt(mean_sq + NORM_EPS) * (1.0 + norm_scale)).astype(jnp.bfloat16)


def rope_tables(positions, head_dim):
    half_dim = head_dim // 2
    inv_freq = ROPE_BASE ** (-2.0 * jnp.arange(half_dim, dtype=jnp.float32) / head_dim)
    angles = positions.astype(jnp.float32)[:, :, None] * inv_freq
    cos_tab, sin_tab = jnp.cos(angles), jnp.sin(angles)
    return jnp.concatenate([cos_tab, cos_tab], axis=-1), jnp.concatenate([-sin_tab, sin_tab], axis=-1)


def attention_body(q_block, pos_row_ref, pos_col_ref, q_ref, k_ref, v_ref, cos_ref, sin_ref, out_ref):
    seq_len, head_dim = q_ref.shape
    half_dim = head_dim // 2

    def rope(states):
        return states * cos_ref[...] + pltpu.roll(states, half_dim, 1) * sin_ref[...]

    keys = rope(k_ref[...]).astype(jnp.bfloat16)
    values = v_ref[...].astype(jnp.bfloat16)
    queries = (rope(q_ref[...]) * QUERY_SCALE).astype(jnp.bfloat16)
    for start in range(0, seq_len, q_block):
        span = start + q_block
        scores = lax.dot_general(queries[start:span], keys[:span], (((1,), (1,)), ((), ())), preferred_element_type=jnp.float32)
        capped = SOFT_CAP * jnp.tanh(scores * (1.0 / SOFT_CAP))
        offset = pos_col_ref[start:span, :] - pos_row_ref[:, :span]
        keep_mask = (offset >= 0) & (offset < WINDOW)
        weights = jnp.where(keep_mask, jnp.exp(capped), 0.0)
        total = jnp.sum(weights, axis=-1, keepdims=True)
        probs = (weights * (1.0 / total)).astype(jnp.bfloat16)
        mix = jnp.dot(probs, values[:span], preferred_element_type=jnp.float32)
        out_ref[start:span, :] = mix.astype(jnp.bfloat16)


def local_attention(qkv, positions, cos_tab, sin_tab, n_heads, head_dim, kv_local):
    seq_len = qkv.shape[0]
    n_group = n_heads // kv_local
    whole = pl.BlockSpec((seq_len, head_dim), lambda h: (0, 0))
    flops = 2 * n_heads * seq_len * seq_len * head_dim * 2
    return pl.pallas_call(
        functools.partial(attention_body, 256),
        grid=(n_heads,),
        in_specs=[
            pl.BlockSpec((1, seq_len), lambda h: (0, 0)),
            pl.BlockSpec((seq_len, 1), lambda h: (0, 0)),
            pl.BlockSpec((seq_len, head_dim), lambda h: (0, h)),
            pl.BlockSpec((seq_len, head_dim), lambda h: (0, n_heads + h // n_group)),
            pl.BlockSpec((seq_len, head_dim), lambda h: (0, n_heads + kv_local + h // n_group)),
            whole,
            whole,
        ],
        out_specs=pl.BlockSpec((seq_len, head_dim), lambda h: (0, h)),
        out_shape=jax.ShapeDtypeStruct((seq_len, n_heads * head_dim), jnp.bfloat16),
        compiler_params=pltpu.CompilerParams(vmem_limit_bytes=40 * 1024 * 1024),
        cost_estimate=pl.CostEstimate(flops=flops, bytes_accessed=12 * seq_len * n_heads * head_dim, transcendentals=0),
        name="attention",
    )(positions[None, :], positions[:, None], qkv, qkv, qkv, cos_tab, sin_tab)


def solution(mesh):
    in_specs = (P("dp", None), P("dp", None), P("tp", None), P(None, "tp", None), P(None, "tp", None), P(None, "tp", None), P("tp", None, None), P(None, "tp"), P(None, "tp"), P("tp", None), P(None), P(None), P(None), P(None))
    n_dev = mesh.shape["tp"]
    n_chip = n_dev // 2
    to_right = [(i, (i + 2) % n_dev) for i in range(n_dev)]
    to_left = [(i, (i - 2) % n_dev) for i in range(n_dev)]
    to_partner = [(i, i ^ 1) for i in range(n_dev)]

    def layer(tokens, positions, embed_block, w_query, w_key, w_value, w_out, w_gate, w_up, w_down, norm_pre_att, norm_post_att, norm_pre_ffw, norm_post_ffw):
        dev_rank = lax.axis_index("tp")
        chip, core = dev_rank // 2, dev_rank % 2
        vocab_local, model_dim = embed_block.shape
        n_batch, seq_len = tokens.shape
        chunk = seq_len // n_dev
        half = chunk // 2
        n_heads, head_dim = w_query.shape[1], w_query.shape[2]
        kv_local = w_key.shape[1]

        clock = []

        def step(fn, *args):
            leaves, tree = jax.tree.flatten(args)
            if clock:
                leaves = lax.optimization_barrier((leaves, list(clock)))[0]
            result = fn(*jax.tree.unflatten(tree, leaves))
            clock[:] = jax.tree.leaves(result)
            return result

        def shift(rows, perm):
            return lax.ppermute(rows, "tp", perm)

        def by_parity(rows, parity):
            split = rows.reshape((n_chip, 2, chunk) + rows.shape[1:])
            picked = lax.dynamic_index_in_dim(split, parity, 1, keepdims=False)
            return picked.reshape((n_chip * chunk,) + rows.shape[1:])

        def ring_steps(own, from_partner, pair_sum, finish):
            def pair(ahead, upper, own, from_partner):
                start = ((chip + ahead) % n_chip) * chunk + (half if upper else 0)
                mine = lax.dynamic_slice_in_dim(own, start, half, 0)
                theirs = lax.dynamic_slice_in_dim(from_partner, start, half, 0)
                return pair_sum(mine, theirs, start, half)

            def first(own, theirs):
                order = ((2, False), (2, True), (1, True), (n_chip - 1, False))
                return [pair(ahead, upper, own, theirs).astype(jnp.bfloat16) for ahead, upper in order]

            sends = step(first, own, from_partner)
            far_low, far_high, left_high, right_low = [shift(part, perm) for part, perm in zip(sends, (to_right, to_left, to_right, to_left))]
            yield

            def second(own, theirs, low, high):
                low = pair(1, False, own, theirs) + low.astype(jnp.float32)
                high = pair(n_chip - 1, True, own, theirs) + high.astype(jnp.float32)
                return low.astype(jnp.bfloat16), high.astype(jnp.bfloat16)

            low, high = step(second, own, from_partner, far_low, far_high)
            left_low, right_high = shift(low, to_right), shift(high, to_left)
            yield

            def last(own, theirs, *arrived):
                right_low, left_low, left_high, right_high = [part.astype(jnp.float32) for part in arrived]
                low = pair(0, False, own, theirs) + right_low + left_low
                high = pair(0, True, own, theirs) + left_high + right_high
                return finish(jnp.concatenate([low, high], axis=0).astype(jnp.bfloat16))

            result = step(last, own, from_partner, right_low, left_low, left_high, right_high)
            yield
            return result

        normalizer = jnp.sqrt(jnp.float32(model_dim)).astype(jnp.bfloat16)
        first_id = dev_rank * vocab_local
        partner_first_id = (dev_rank + 1 - 2 * core) * vocab_local

        def lookup(ids):
            return embed_block.at[jnp.mod(ids - first_id, vocab_local)].get(mode="promise_in_bounds")

        w_qkv = jnp.concatenate([w.reshape(model_dim, -1) for w in (w_query, w_key, w_value)], axis=1)
        w_out_flat = w_out.reshape(-1, model_dim)
        cos_tab, sin_tab = rope_tables(positions, head_dim)

        def project_out(rows):
            return jnp.dot(rows, w_out_flat, preferred_element_type=jnp.float32).astype(jnp.bfloat16)

        def project_down(rows):
            return jnp.dot(rows, w_down, preferred_element_type=jnp.float32).astype(jnp.bfloat16)

        def add_sums(mine, theirs, start, size):
            return mine.astype(jnp.float32) + theirs.astype(jnp.float32)

        def row_steps(b):
            own_ids, other_ids = by_parity(tokens[b], core), by_parity(tokens[b], 1 - core)
            other = step(lookup, other_ids)
            from_partner = shift(other, to_partner)
            yield
            own = step(lookup, own_ids)
            yield

            def pick_row(mine, theirs, start, size):
                ids = lax.dynamic_slice_in_dim(own_ids, start, size, 0)[:, None]
                from_mine = (ids >= first_id) & (ids < first_id + vocab_local)
                from_theirs = (ids >= partner_first_id) & (ids < partner_first_id + vocab_local)
                zero = jnp.zeros((), jnp.bfloat16)
                return jnp.where(from_mine, mine * normalizer, jnp.where(from_theirs, theirs * normalizer, zero)).astype(jnp.float32)

            embeds, normed = yield from ring_steps(own, from_partner, pick_row, lambda e: (e, rms_norm(e, norm_pre_att)))
            attn_in = lax.all_gather(normed, "tp", axis=0, tiled=True)
            qkv = step(lambda rows: jnp.dot(rows, w_qkv, preferred_element_type=jnp.float32), attn_in)
            yield
            att_mix = step(lambda rows: local_attention(rows, positions[b], cos_tab[b], sin_tab[b], n_heads, head_dim, kv_local), qkv)
            yield
            other = step(lambda rows: project_out(by_parity(rows, 1 - core)), att_mix)
            from_partner = shift(other, to_partner)
            yield
            own = step(lambda rows: project_out(by_parity(rows, core)), att_mix)
            yield

            def after_attention(att_proj):
                resid = (embeds.astype(jnp.float32) + rms_norm(att_proj, norm_post_att).astype(jnp.float32)).astype(jnp.bfloat16)
                return resid, rms_norm(resid, norm_pre_ffw)

            resid_one, normed = yield from ring_steps(own, from_partner, add_sums, after_attention)
            mlp_in = lax.all_gather(normed, "tp", axis=0, tiled=True)
            gate_pre = step(lambda rows: jnp.dot(rows, w_gate, preferred_element_type=jnp.float32), mlp_in)
            yield

            def activate(rows, gate_pre):
                up_proj = jnp.dot(rows, w_up, preferred_element_type=jnp.float32)
                return (jax.nn.gelu(gate_pre, approximate=True) * up_proj).astype(jnp.bfloat16)

            ffn_act = step(activate, mlp_in, gate_pre)
            yield
            other = step(lambda rows: project_down(by_parity(rows, 1 - core)), ffn_act)
            from_partner = shift(other, to_partner)
            yield
            own = step(lambda rows: project_down(by_parity(rows, core)), ffn_act)
            yield

            def after_ffw(down_proj):
                return (resid_one.astype(jnp.float32) + rms_norm(down_proj, norm_post_ffw).astype(jnp.float32)).astype(jnp.bfloat16)

            outs[b] = yield from ring_steps(own, from_partner, add_sums, after_ffw)

        outs = [None] * n_batch
        rows = [row_steps(b) for b in range(n_batch)]
        for b in step_order(n_batch):
            next(rows[b], None)
        for row in rows:
            for _ in row:
                pass
        return jnp.stack(outs)

    return jax.shard_map(layer, mesh=mesh, in_specs=in_specs, out_specs=P("dp", "tp", None), check_vma=False)
```

```python
import functools

import jax
import jax.numpy as jnp
from jax import lax
from jax.experimental import pallas as pl
from jax.experimental.pallas import tpu as pltpu
from jax.sharding import PartitionSpec as P


WINDOW = 4096
QUERY_SCALE = 256.0 ** -0.5
SOFT_CAP = 50.0
NORM_EPS = 1e-6
ROPE_BASE = 10000.0

ROW_ORDER = "000101120212100000021012111010012222202121110210221220122"


def step_order(n_batch):
    return [int(row) for row in ROW_ORDER if int(row) < n_batch]


def rms_norm(hidden, norm_scale):
    hidden = hidden.astype(jnp.float32)
    mean_sq = jnp.mean(hidden * hidden, axis=-1, keepdims=True)
    return (hidden * lax.rsqrt(mean_sq + NORM_EPS) * (1.0 + norm_scale)).astype(jnp.bfloat16)


def rope_tables(positions, head_dim):
    half_dim = head_dim // 2
    inv_freq = ROPE_BASE ** (-2.0 * jnp.arange(half_dim, dtype=jnp.float32) / head_dim)
    angles = positions.astype(jnp.float32)[:, :, None] * inv_freq
    cos_tab, sin_tab = jnp.cos(angles), jnp.sin(angles)
    return jnp.concatenate([cos_tab, cos_tab], axis=-1), jnp.concatenate([-sin_tab, sin_tab], axis=-1)


def attention_body(q_block, pos_row_ref, pos_col_ref, q_ref, k_ref, v_ref, cos_ref, sin_ref, out_ref):
    seq_len, head_dim = q_ref.shape
    half_dim = head_dim // 2

    def rope(states):
        return states * cos_ref[...] + pltpu.roll(states, half_dim, 1) * sin_ref[...]

    keys = rope(k_ref[...]).astype(jnp.bfloat16)
    values = v_ref[...].astype(jnp.bfloat16)
    queries = (rope(q_ref[...]) * QUERY_SCALE).astype(jnp.bfloat16)
    for start in range(0, seq_len, q_block):
        span = start + q_block
        scores = lax.dot_general(queries[start:span], keys[:span], (((1,), (1,)), ((), ())), preferred_element_type=jnp.float32)
        capped = SOFT_CAP * jnp.tanh(scores * (1.0 / SOFT_CAP))
        offset = pos_col_ref[start:span, :] - pos_row_ref[:, :span]
        keep_mask = (offset >= 0) & (offset < WINDOW)
        weights = jnp.where(keep_mask, jnp.exp(capped), 0.0)
        total = jnp.sum(weights, axis=-1, keepdims=True)
        probs = (weights * (1.0 / total)).astype(jnp.bfloat16)
        mix = jnp.dot(probs, values[:span], preferred_element_type=jnp.float32)
        out_ref[start:span, :] = mix.astype(jnp.bfloat16)


def local_attention(qkv, positions, cos_tab, sin_tab, n_heads, head_dim, kv_local):
    seq_len = qkv.shape[0]
    n_group = n_heads // kv_local
    whole = pl.BlockSpec((seq_len, head_dim), lambda h: (0, 0))
    flops = 2 * n_heads * seq_len * seq_len * head_dim * 2
    return pl.pallas_call(
        functools.partial(attention_body, 256),
        grid=(n_heads,),
        in_specs=[
            pl.BlockSpec((1, seq_len), lambda h: (0, 0)),
            pl.BlockSpec((seq_len, 1), lambda h: (0, 0)),
            pl.BlockSpec((seq_len, head_dim), lambda h: (0, h)),
            pl.BlockSpec((seq_len, head_dim), lambda h: (0, n_heads + h // n_group)),
            pl.BlockSpec((seq_len, head_dim), lambda h: (0, n_heads + kv_local + h // n_group)),
            whole,
            whole,
        ],
        out_specs=pl.BlockSpec((seq_len, head_dim), lambda h: (0, h)),
        out_shape=jax.ShapeDtypeStruct((seq_len, n_heads * head_dim), jnp.bfloat16),
        compiler_params=pltpu.CompilerParams(vmem_limit_bytes=40 * 1024 * 1024),
        cost_estimate=pl.CostEstimate(flops=flops, bytes_accessed=12 * seq_len * n_heads * head_dim, transcendentals=0),
        name="attention",
    )(positions[None, :], positions[:, None], qkv, qkv, qkv, cos_tab, sin_tab)


def gate_up_body(parity_ref, rows_ref, gate_ref, up_ref, out_ref):
    rows = rows_ref[...].reshape(out_ref.shape[0], rows_ref.shape[-1])
    gate = jnp.dot(rows, gate_ref[...], preferred_element_type=jnp.float32)
    up_proj = jnp.dot(rows, up_ref[...], preferred_element_type=jnp.float32)
    out_ref[...] = (jax.nn.gelu(gate, approximate=True) * up_proj).astype(jnp.bfloat16)


def gate_up(rows, parity, w_gate, w_up, chunk):
    seq_len, model_dim = rows.shape
    width = w_gate.shape[1]
    n_pair, col_tile = seq_len // (2 * chunk), 256
    out_rows = n_pair * chunk
    return pl.pallas_call(
        gate_up_body,
        grid_spec=pltpu.PrefetchScalarGridSpec(
            num_scalar_prefetch=1,
            grid=(width // col_tile,),
            in_specs=[
                pl.BlockSpec((n_pair, None, chunk, model_dim), lambda j, parity: (0, parity[0], 0, 0)),
                pl.BlockSpec((model_dim, col_tile), lambda j, parity: (0, j)),
                pl.BlockSpec((model_dim, col_tile), lambda j, parity: (0, j)),
            ],
            out_specs=pl.BlockSpec((out_rows, col_tile), lambda j, parity: (0, j)),
        ),
        out_shape=jax.ShapeDtypeStruct((out_rows, width), jnp.bfloat16),
        compiler_params=pltpu.CompilerParams(vmem_limit_bytes=40 * 1024 * 1024),
        cost_estimate=pl.CostEstimate(flops=4 * out_rows * model_dim * width, bytes_accessed=4 * model_dim * width, transcendentals=0),
        name="gate_up",
    )(parity.reshape(1).astype(jnp.int32), rows.reshape(n_pair, 2, chunk, model_dim), w_gate, w_up)


def solution(mesh):
    in_specs = (P("dp", None), P("dp", None), P("tp", None), P(None, "tp", None), P(None, "tp", None), P(None, "tp", None), P("tp", None, None), P(None, "tp"), P(None, "tp"), P("tp", None), P(None), P(None), P(None), P(None))
    n_dev = mesh.shape["tp"]
    n_chip = n_dev // 2
    to_right = [(i, (i + 2) % n_dev) for i in range(n_dev)]
    to_left = [(i, (i - 2) % n_dev) for i in range(n_dev)]
    to_partner = [(i, i ^ 1) for i in range(n_dev)]

    def layer(tokens, positions, embed_block, w_query, w_key, w_value, w_out, w_gate, w_up, w_down, norm_pre_att, norm_post_att, norm_pre_ffw, norm_post_ffw):
        dev_rank = lax.axis_index("tp")
        chip, core = dev_rank // 2, dev_rank % 2
        vocab_local, model_dim = embed_block.shape
        n_batch, seq_len = tokens.shape
        chunk = seq_len // n_dev
        half = chunk // 2
        n_heads, head_dim = w_query.shape[1], w_query.shape[2]
        kv_local = w_key.shape[1]

        clock = []

        def step(fn, *args):
            leaves, tree = jax.tree.flatten(args)
            if clock:
                leaves = lax.optimization_barrier((leaves, list(clock)))[0]
            result = fn(*jax.tree.unflatten(tree, leaves))
            clock[:] = jax.tree.leaves(result)
            return result

        def shift(rows, perm):
            return lax.ppermute(rows, "tp", perm)

        def by_parity(rows, parity):
            split = rows.reshape((n_chip, 2, chunk) + rows.shape[1:])
            picked = lax.dynamic_index_in_dim(split, parity, 1, keepdims=False)
            return picked.reshape((n_chip * chunk,) + rows.shape[1:])

        def ring_steps(own, from_partner, pair_sum, finish):
            def pair(ahead, upper, own, from_partner):
                start = ((chip + ahead) % n_chip) * chunk + (half if upper else 0)
                mine = lax.dynamic_slice_in_dim(own, start, half, 0)
                theirs = lax.dynamic_slice_in_dim(from_partner, start, half, 0)
                return pair_sum(mine, theirs, start, half)

            def first(own, theirs):
                order = ((2, False), (2, True), (1, True), (n_chip - 1, False))
                return [pair(ahead, upper, own, theirs).astype(jnp.bfloat16) for ahead, upper in order]

            sends = step(first, own, from_partner)
            far_low, far_high, left_high, right_low = [shift(part, perm) for part, perm in zip(sends, (to_right, to_left, to_right, to_left))]
            yield

            def second(own, theirs, low, high):
                low = pair(1, False, own, theirs) + low.astype(jnp.float32)
                high = pair(n_chip - 1, True, own, theirs) + high.astype(jnp.float32)
                return low.astype(jnp.bfloat16), high.astype(jnp.bfloat16)

            low, high = step(second, own, from_partner, far_low, far_high)
            left_low, right_high = shift(low, to_right), shift(high, to_left)
            yield

            def last(own, theirs, *arrived):
                right_low, left_low, left_high, right_high = [part.astype(jnp.float32) for part in arrived]
                low = pair(0, False, own, theirs) + right_low + left_low
                high = pair(0, True, own, theirs) + left_high + right_high
                return finish(jnp.concatenate([low, high], axis=0).astype(jnp.bfloat16))

            result = step(last, own, from_partner, right_low, left_low, left_high, right_high)
            yield
            return result

        normalizer = jnp.sqrt(jnp.float32(model_dim)).astype(jnp.bfloat16)
        first_id = dev_rank * vocab_local
        partner_first_id = (dev_rank + 1 - 2 * core) * vocab_local

        def lookup(ids):
            return embed_block.at[jnp.mod(ids - first_id, vocab_local)].get(mode="promise_in_bounds")

        w_qkv = jnp.concatenate([w.reshape(model_dim, -1) for w in (w_query, w_key, w_value)], axis=1)
        w_out_flat = w_out.reshape(-1, model_dim)
        cos_tab, sin_tab = rope_tables(positions, head_dim)

        def project_out(rows):
            return jnp.dot(rows, w_out_flat, preferred_element_type=jnp.float32).astype(jnp.bfloat16)

        def project_down(rows):
            return jnp.dot(rows, w_down, preferred_element_type=jnp.float32).astype(jnp.bfloat16)

        def add_sums(mine, theirs, start, size):
            return mine.astype(jnp.float32) + theirs.astype(jnp.float32)

        def row_steps(b):
            own_ids, other_ids = by_parity(tokens[b], core), by_parity(tokens[b], 1 - core)
            other = step(lookup, other_ids)
            from_partner = shift(other, to_partner)
            yield
            own = step(lookup, own_ids)
            yield

            def pick_row(mine, theirs, start, size):
                ids = lax.dynamic_slice_in_dim(own_ids, start, size, 0)[:, None]
                from_mine = (ids >= first_id) & (ids < first_id + vocab_local)
                from_theirs = (ids >= partner_first_id) & (ids < partner_first_id + vocab_local)
                zero = jnp.zeros((), jnp.bfloat16)
                return jnp.where(from_mine, mine * normalizer, jnp.where(from_theirs, theirs * normalizer, zero)).astype(jnp.float32)

            embeds, normed = yield from ring_steps(own, from_partner, pick_row, lambda e: (e, rms_norm(e, norm_pre_att)))
            attn_in = lax.all_gather(normed, "tp", axis=0, tiled=True)
            qkv = step(lambda rows: jnp.dot(rows, w_qkv, preferred_element_type=jnp.float32), attn_in)
            yield
            att_mix = step(lambda rows: local_attention(rows, positions[b], cos_tab[b], sin_tab[b], n_heads, head_dim, kv_local), qkv)
            yield
            other = step(lambda rows: project_out(by_parity(rows, 1 - core)), att_mix)
            from_partner = shift(other, to_partner)
            yield
            own = step(lambda rows: project_out(by_parity(rows, core)), att_mix)
            yield

            def after_attention(att_proj):
                resid = (embeds.astype(jnp.float32) + rms_norm(att_proj, norm_post_att).astype(jnp.float32)).astype(jnp.bfloat16)
                return resid, rms_norm(resid, norm_pre_ffw)

            resid_one, normed = yield from ring_steps(own, from_partner, add_sums, after_attention)
            mlp_in = lax.all_gather(normed, "tp", axis=0, tiled=True)
            other_act = step(lambda rows: gate_up(rows, 1 - core, w_gate, w_up, chunk), mlp_in)
            yield
            other = step(project_down, other_act)
            from_partner = shift(other, to_partner)
            yield
            own_act = step(lambda rows: gate_up(rows, core, w_gate, w_up, chunk), mlp_in)
            yield
            own = step(project_down, own_act)
            yield

            def after_ffw(down_proj):
                return (resid_one.astype(jnp.float32) + rms_norm(down_proj, norm_post_ffw).astype(jnp.float32)).astype(jnp.bfloat16)

            outs[b] = yield from ring_steps(own, from_partner, add_sums, after_ffw)

        outs = [None] * n_batch
        rows = [row_steps(b) for b in range(n_batch)]
        for b in step_order(n_batch):
            next(rows[b], None)
        for row in rows:
            for _ in row:
                pass
        return jnp.stack(outs)

    return jax.shard_map(layer, mesh=mesh, in_specs=in_specs, out_specs=P("dp", "tp", None), check_vma=False)
```
